32 devices in a mesh: row: 4 (over y, x), col: 8 (over z, core).
Axes of the slice: x: 2, y: 2, z: 4, core: 2. Of those that a mesh axis runs over, the one named last changes fastest.
Arguments:
- activations: bfloat16 [1024, 9216], P('col', 'row'), may hold values from -64 to 64
- output_grads: bfloat16 [1024, 73728], P('row', 'col'), may hold values from -16 to 16
- weight: bfloat16 [9216, 73728], P('row', 'col'), may hold values from -1 to 1
- row_moment: float32 [9216], P('row'), may hold values from 0.01 to 0.3
- col_moment: float32 [73728], P('col'), may hold values from 0.01 to 0.3
Outputs:
- new_weight: bfloat16 [9216, 73728], P('row', 'col')
- new_row: float32 [9216], P('row')
- new_col: float32 [73728], P('col')
The draws below stay inside these ranges and needn't reach their ends.
All inputs are finite; a program needn't handle non-finite values.
Results may differ from the reference program's by a relative error of at most 0.0004.
Values may be sent and summed in bfloat16 or wider, within the bound.
A program may use at most 256 MiB of HBM per device.

```python
import math
import jax
import jax.numpy as jnp
from jax import lax

D = 9216
FF = 73728
TOKENS = 1024


def scales(key, length, trend, spread):
    position = jnp.arange(length, dtype=jnp.float32) / length
    jitter = jax.random.uniform(key, (length,), jnp.float32, 0.0, math.log(spread))
    return jnp.exp(math.log(trend) * position + jitter)


def shaped_panel(key, rows_total, width, divisor):
    keys = jax.random.split(key, 2)
    values = jax.random.normal(keys[0], (rows_total, width), jnp.float32)
    factor = scales(keys[1], width, 3.0, 10.0) / 4.0
    return values * factor[None, :] / divisor


def draw_activations(key, part):
    values = shaped_panel(jax.random.fold_in(key, 11), TOKENS, D, 1.0)
    return jnp.clip(values, -64.0, 64.0).astype(jnp.bfloat16)


def draw_output_grads(key, part):
    values = shaped_panel(jax.random.fold_in(key, 23), TOKENS, FF, math.sqrt(TOKENS))
    return jnp.clip(values, -16.0, 16.0).astype(jnp.bfloat16)


def draw_weight(key, part):
    keys = jax.random.split(jax.random.fold_in(key, 37), 3)
    values = jax.random.normal(keys[0], (D, FF), jnp.float32)
    row_scale = scales(keys[1], D, 3.0, 10.0) / 4.0
    col_scale = scales(keys[2], FF, 3.0, 10.0) / 4.0
    values = values * row_scale[:, None] * col_scale[None, :] / math.sqrt(D)
    return jnp.clip(values, -1.0, 1.0).astype(jnp.bfloat16)


def steps_of(key, shape, cuts, low, top_value):
    loudness, own = 1.0, jax.random.fold_in(key, 6)
    for axis_at, shards_of in cuts:
        draws = jnp.exp(jax.random.uniform(jax.random.fold_in(own, axis_at), (shards_of,), jnp.float32, low / len(cuts), top_value / len(cuts)))
        loudness = loudness * jnp.repeat(draws, shape[axis_at] // shards_of).reshape([-1 if axis == axis_at else 1 for axis in range(len(shape))])
    return loudness


def setup_inputs(seed: int = 0) -> dict:
    streams_of = jax.random.split(jax.random.key(seed), 6)
    return {
        "activations": draw_activations(jax.random.fold_in(streams_of[5], 71), 0),
        "output_grads": draw_output_grads(jax.random.fold_in(streams_of[5], 71), 0),
        "weight": draw_weight(jax.random.fold_in(streams_of[5], 71), 0),
        "row_moment": jnp.clip(jnp.exp(math.log(0.3) - 3.4011974 * jax.random.uniform(streams_of[3], (D,), jnp.float32) ** steps_of(streams_of[3], (D,), ((0, 4),), -0.2, 0.2)), 0.01, 0.3),
        "col_moment": jnp.clip(jnp.exp(math.log(0.3) - 3.4011974 * jax.random.uniform(streams_of[4], (FF,), jnp.float32) ** steps_of(streams_of[4], (FF,), ((0, 8),), -0.2, 0.2)), 0.01, 0.3),
    }


ADDED_SQUARE = 1e-30
DECAY_RATE = 0.8
CLIP_LIMIT = 1.0
STEP_SIZE = 0.1
MEAN_OFFSET = 1e-06

def reference(activations, output_grads, weight, row_moment, col_moment):
    block_rows = math.gcd(D, 1152)
    block_count = D // block_rows
    left_side = activations.astype(jnp.float32).T.reshape(block_count, block_rows, TOKENS)
    right_side = output_grads.astype(jnp.float32)
    weight_blocks = weight.reshape(block_count, block_rows, FF)

    def grad_block(left_block):
        return jnp.dot(left_block, right_side, preferred_element_type=jnp.float32)

    def first_pass(carry, left_block):
        squared = jnp.square(grad_block(left_block)) + ADDED_SQUARE
        return (carry + lax.optimization_barrier(jnp.sum(squared, axis=0)), lax.optimization_barrier(jnp.sum(squared, axis=1)))
    col_total, row_total = lax.scan(first_pass, jnp.zeros((FF,), jnp.float32), left_side)
    new_row = DECAY_RATE * row_moment + (1.0 - DECAY_RATE) * row_total.reshape(D) / FF
    new_col = DECAY_RATE * col_moment + (1.0 - DECAY_RATE) * col_total / D
    row_mean = jnp.sum(new_row) / D
    row_blocks = new_row.reshape(block_count, block_rows)

    def update_block(left_block, row_block):
        return grad_block(left_block) / jnp.sqrt(row_block[:, None] * new_col[None, :] / row_mean)

    def second_pass(carry, items):
        left_block, row_block, weight_block = items
        update = update_block(left_block, row_block)
        widened = weight_block.astype(jnp.float32)
        return ((carry[0] + jnp.sum(update * update), carry[1] + jnp.sum(widened * widened)), None)
    start = (jnp.zeros((), jnp.float32), jnp.zeros((), jnp.float32))
    (update_total, weight_total), _ = lax.scan(second_pass, start, (left_side, row_blocks, weight_blocks))
    entries = float(D * FF)
    clip_factor = jnp.maximum(1.0, jnp.sqrt(update_total / entries) / CLIP_LIMIT)
    step_scale = STEP_SIZE * jnp.sqrt(weight_total / entries + MEAN_OFFSET)

    def third_pass(items):
        left_block, row_block, weight_block = items
        update = update_block(left_block, row_block)
        return (weight_block.astype(jnp.float32) - step_scale / clip_factor * update).astype(jnp.bfloat16)
    new_weight = lax.map(third_pass, (left_side, row_blocks, weight_blocks)).reshape(D, FF)
    return (new_weight, new_row, new_col)
```

```python
import functools

import jax
import jax.numpy as jnp
from jax import lax
from jax.experimental import pallas as pl
from jax.experimental.pallas import tpu as pltpu
from jax.sharding import PartitionSpec as P

ADDED_SQUARE = 1e-30
DECAY_RATE = 0.8
CLIP_LIMIT = 1.0
STEP_SIZE = 0.1
MEAN_OFFSET = 1e-06

MESH = pl.DeviceIdType.MESH
WIDTH = 512
TALL = 768
KEPT = 192
SUB = 256
AHEAD = 2
LAG = 2
SLOTS = LAG + 1
ACTS_FORWARD = 3
ACTS_READY = 5


def lane_sum(x):
    out = x[:, :128]
    for k in range(1, x.shape[1] // 128):
        out = out + x[:, k * 128 : (k + 1) * 128]
    return out


def sublane_sum(x):
    return jnp.sum(x.reshape(x.shape[0] // 8, 8, x.shape[1]), axis=0)


def gather_kernel(
    rows, cols,
    acts_ref, og_ref, w_ref, rm_ref, cm_ref,
    og_out, at_out, g_out, nr_out, nc_out, rs_out, cs_out,
    og_all, acts_all, acts_t, grad, wbuf, rowacc, sacc, wacc, colx, rowx, scb, scc,
    load_sem, og_sem, acts_sem, sib_sem, col_sem, row_sem, scb_sem, scc_sem, w_sem, out_sem, g_sem, misc_sem,
):
    n, tokens, width = og_all.shape
    tile_rows = acts_t.shape[0]
    blocks = tile_rows // TALL
    share = tokens // rows
    half = share // 2
    wrows = tile_rows // n
    total_rows = tile_rows * rows
    total_cols = n * width * cols
    entries = float(total_rows * total_cols)
    r, c = lax.axis_index("row"), lax.axis_index("col")
    rx = r + 1 - 2 * lax.rem(r, 2)
    ry = lax.rem(r + 2, 4)
    rd = lax.rem(rx + 2, 4)
    sib = c + 1 - 2 * lax.rem(c, 2)

    def region(owner, start, size):
        return pl.ds(pl.multiple_of(owner * share + start, half), size)

    def load(j):
        return pltpu.make_async_copy(
            og_ref.at[:, pl.ds(pl.multiple_of(j * width, width), width)],
            og_all.at[j, region(r, 0, share), :], load_sem.at[j])

    def og_copy(j, kind, owner, start, size, to):
        ref = og_all.at[j, region(owner, start, size), :]
        return pltpu.make_async_remote_copy(
            src_ref=ref, dst_ref=ref, send_sem=og_sem.at[0, kind, j], recv_sem=og_sem.at[1, kind, j],
            device_id={"row": to}, device_id_type=MESH)

    def own_x(j):
        return og_copy(j, 0, r, 0, share, rx)

    def own_y(j):
        return og_copy(j, 1, r, 0, share, ry)

    def fwd_y(j):
        return og_copy(j, 2, rx, 0, half, ry)

    def fwd_x(j):
        return og_copy(j, 3, ry, half, half, rx)

    def acts_copy(d):
        to = lax.rem(c + 2 * d, cols)
        return pltpu.make_async_remote_copy(
            src_ref=acts_all.at[c], dst_ref=acts_all.at[c], send_sem=acts_sem.at[0, d], recv_sem=acts_sem.at[1, d],
            device_id={"col": to}, device_id_type=MESH)

    def sib_copy(d):
        at = lax.rem(c + cols - 2 * d, cols)
        return pltpu.make_async_remote_copy(
            src_ref=acts_all.at[at], dst_ref=acts_all.at[at], send_sem=sib_sem.at[0, d], recv_sem=sib_sem.at[1, d],
            device_id={"col": sib}, device_id_type=MESH)

    def col_copy(j, d):
        return pltpu.make_async_remote_copy(
            src_ref=colx.at[r, j], dst_ref=colx.at[r, j], send_sem=col_sem.at[0, d, j], recv_sem=col_sem.at[1, d, j],
            device_id={"row": lax.rem(r + d, rows)}, device_id_type=MESH)

    def row_copy(d):
        return pltpu.make_async_remote_copy(
            src_ref=rowx.at[c], dst_ref=rowx.at[c], send_sem=row_sem.at[0, d], recv_sem=row_sem.at[1, d],
            device_id={"col": lax.rem(c + d, cols)}, device_id_type=MESH)

    def scb_copy(d):
        return pltpu.make_async_remote_copy(
            src_ref=scb.at[c], dst_ref=scb.at[c], send_sem=scb_sem.at[0, d], recv_sem=scb_sem.at[1, d],
            device_id={"col": lax.rem(c + d, cols)}, device_id_type=MESH)

    def scc_copy(d):
        return pltpu.make_async_remote_copy(
            src_ref=scc.at[r], dst_ref=scc.at[r], send_sem=scc_sem.at[0, d], recv_sem=scc_sem.at[1, d],
            device_id={"row": lax.rem(r + d, rows)}, device_id_type=MESH)

    def w_copy(j):
        return pltpu.make_async_copy(
            w_ref.at[pl.ds(pl.multiple_of(j * wrows, wrows), wrows), :], wbuf.at[lax.rem(j, 2)], w_sem.at[lax.rem(j, 2)])

    def og_store(j):
        return pltpu.make_async_copy(og_all.at[j], og_out.at[j], out_sem.at[j])

    def g_store(j):
        s = lax.rem(j, SLOTS)
        return pltpu.make_async_copy(grad.at[s, :, pl.ds(TALL - KEPT, KEPT), :], g_out.at[j], g_sem.at[s])

    acts_load = pltpu.make_async_copy(acts_ref, acts_all.at[c], misc_sem.at[0])
    acts_store = pltpu.make_async_copy(acts_t, at_out, misc_sem.at[1])

    acts_load.start()

    @pl.loop(0, n)
    def _(j):
        load(j).start()

    w_copy(0).start()
    w_copy(1).start()

    barrier = pltpu.get_barrier_semaphore()
    for d in range(1, rows):
        pl.semaphore_signal(barrier, inc=1, device_id={"row": lax.rem(r + d, rows)}, device_id_type=MESH)
    for d in range(1, cols):
        pl.semaphore_signal(barrier, inc=1, device_id={"col": lax.rem(c + d, cols)}, device_id_type=MESH)
    rowacc[...] = jnp.zeros_like(rowacc)
    sacc[...] = jnp.zeros_like(sacc)
    wacc[...] = jnp.zeros_like(wacc)
    pl.semaphore_wait(barrier, rows + cols - 2)

    def send_own(j):
        load(j).wait()
        own_x(j).start()
        own_y(j).start()

    for j in range(AHEAD):
        send_own(j)
    acts_load.wait()
    for d in range(1, cols // 2):
        acts_copy(d).start()
    sib_copy(0).start()

    def exchange(j):
        own_x(j).wait_recv()
        fwd_y(j).start()
        own_y(j).wait_recv()
        fwd_x(j).start()

        @pl.when(j + AHEAD < n)
        def _():
            send_own(j + AHEAD)

    def weigh(j):
        w_copy(j).wait()
        s = lax.rem(j, 2)
        wide = 1024

        @pl.loop(0, wbuf.shape[2] // wide)
        def _(k):
            x = wbuf[s, :, pl.ds(pl.multiple_of(k * wide, wide), wide)].astype(jnp.float32)
            wacc[...] += sublane_sum(x * x)

        @pl.when(j + 2 < n)
        def _():
            w_copy(j + 2).start()

    def stats(k):
        for d in range(1, rows):
            col_copy(k, d).wait_recv()
        total = colx[0, k]
        for q in range(1, rows):
            total = total + colx[q, k]
        factor = DECAY_RATE * cm_ref[k] + (1.0 - DECAY_RATE) * total / total_rows
        nc_out[k] = factor
        cs_out[k] = lax.rsqrt(factor)
        weight = 1.0 / factor
        s = lax.rem(k, SLOTS)
        for b in range(blocks):
            @pl.loop(0, TALL // SUB)
            def _(i):
                at = pl.ds(pl.multiple_of(i * SUB, SUB), SUB)
                g = grad[s, b, at, :]
                to = pl.ds(pl.multiple_of(b * TALL + i * SUB, SUB), SUB)
                sacc[to, :] += lane_sum(g * g * weight)

    def compute(k):
        fwd_y(k).wait_recv()
        fwd_x(k).wait_recv()
        og_store(k).start()
        s = lax.rem(k, SLOTS)

        @pl.when(k >= SLOTS)
        def _():
            g_store(k - SLOTS).wait()

        right = og_all.at[k]
        column = jnp.zeros((8, width), jnp.float32)
        for b in range(blocks):
            def step(i, column):
                to = pl.ds(pl.multiple_of(b * TALL + i * SUB, SUB), SUB)
                g = jnp.dot(acts_t[to, :], right[...], preferred_element_type=jnp.float32)
                grad[s, b, pl.ds(pl.multiple_of(i * SUB, SUB), SUB), :] = g
                squared = g * g + ADDED_SQUARE
                rowacc[to, :] += lane_sum(squared)
                return column + sublane_sum(squared)
            column = lax.fori_loop(0, TALL // SUB, step, column)
        colx[r, k] = jnp.sum(column, axis=0, keepdims=True)
        for d in range(1, rows):
            col_copy(k, d).start()
        g_store(k).start()

        @pl.when(k >= LAG)
        def _():
            stats(k - LAG)

    def reach(j):
        return jnp.minimum(j, 2 * (j - ACTS_READY + 1))

    @pl.loop(0, ACTS_FORWARD)
    def _(j):
        exchange(j)
        weigh(j)

    for d in range(1, cols // 2):
        acts_copy(d).wait_recv()
        sib_copy(d).start()

    @pl.loop(ACTS_FORWARD, ACTS_READY)
    def _(j):
        exchange(j)
        weigh(j)

    for d in range(cols // 2):
        sib_copy(d).wait_recv()
    part = acts_all.shape[1]
    for q in range(cols):
        acts_t[:, q * part : (q + 1) * part] = acts_all[q].T
    acts_store.start()

    @pl.loop(ACTS_READY, n)
    def _(j):
        exchange(j)
        weigh(j)

        @pl.loop(reach(j - 1), reach(j))
        def _(k):
            compute(k)

    @pl.loop(n - 1, n)
    def _(k):
        compute(k)

    rowx[c] = jnp.sum(rowacc[...].T, axis=0, keepdims=True)
    for d in range(1, cols):
        row_copy(d).start()

    @pl.loop(n - LAG, n)
    def _(k):
        stats(k)

    ratio_rows = jnp.sum(sacc[...].T, axis=0, keepdims=True)
    for d in range(1, cols):
        row_copy(d).wait_recv()
    row_total = rowx[0]
    for q in range(1, cols):
        row_total = row_total + rowx[q]
    new_row = DECAY_RATE * rm_ref[...] + (1.0 - DECAY_RATE) * row_total / total_cols
    nr_out[...] = new_row

    def spread(x):
        return jnp.broadcast_to(jnp.sum(x, axis=1, keepdims=True), (1, 128))

    scb[c, 0:1, :] = spread(ratio_rows / new_row)
    scb[c, 1:2, :] = spread(jnp.sum(wacc[...], axis=0, keepdims=True))
    for d in range(1, cols):
        scb_copy(d).start()
    row_sum = spread(new_row)
    for d in range(1, cols):
        scb_copy(d).wait_recv()
    both = scb[0]
    for q in range(1, cols):
        both = both + scb[q]
    scc[r, 0:2, :] = both[0:2, :]
    scc[r, 2:3, :] = row_sum
    for d in range(1, rows):
        scc_copy(d).start()
    root = lax.rsqrt(new_row)
    for d in range(1, rows):
        scc_copy(d).wait_recv()
    every = scc[0]
    for q in range(1, rows):
        every = every + scc[q]
    row_mean = every[2:3, :] / total_rows
    rms_update = jnp.sqrt(row_mean * (every[0:1, :] / entries))
    clip_factor = jnp.maximum(1.0, rms_update / CLIP_LIMIT)
    step_scale = STEP_SIZE * jnp.sqrt(every[1:2, :] / entries + MEAN_OFFSET)
    scale = step_scale / clip_factor * jnp.sqrt(row_mean)
    rs_out[...] = jnp.broadcast_to(root, (128, tile_rows)).T * scale

    @pl.loop(0, n)
    def _(j):
        own_x(j).wait_send()
        own_y(j).wait_send()
        fwd_y(j).wait_send()
        fwd_x(j).wait_send()
        og_store(j).wait()
        for d in range(1, rows):
            col_copy(j, d).wait_send()

    @pl.loop(n - SLOTS, n)
    def _(j):
        g_store(j).wait()

    acts_store.wait()
    for d in range(1, cols // 2):
        acts_copy(d).wait_send()
    for d in range(cols // 2):
        sib_copy(d).wait_send()
    for d in range(1, cols):
        row_copy(d).wait_send()
        scb_copy(d).wait_send()
    for d in range(1, rows):
        scc_copy(d).wait_send()


def update_kernel(at_ref, og_ref, w_ref, g_ref, rs_ref, cs_ref, out_ref):
    i = pl.program_id(1)
    tall, width = w_ref.shape
    cs = cs_ref[0]
    sub = KEPT

    def finish(g, at):
        rs = rs_ref[at, :]
        wide = jnp.concatenate([rs] * (width // 128), axis=1)
        out_ref[at, :] = (w_ref[at, :].astype(jnp.float32) - g * wide * cs).astype(out_ref.dtype)

    finish(g_ref[0, 0], pl.ds(tall - KEPT, KEPT))
    for k in range((tall - KEPT) // sub):
        left = at_ref[pl.ds(pl.multiple_of(i * tall + k * sub, sub), sub), :]
        g = jnp.dot(left, og_ref[0], preferred_element_type=jnp.float32)
        finish(g, pl.ds(k * sub, sub))


def with_kernels(rows, cols, activations, output_grads, weight, row_moment, col_moment):
    tile_rows, tile_cols = weight.shape
    part = activations.shape[0]
    tokens = part * cols
    n, width = tile_cols // WIDTH, WIDTH
    blocks = tile_rows // TALL
    f32, bf16 = jnp.float32, jnp.bfloat16
    any_space = pl.BlockSpec(memory_space=pl.ANY)
    vmem = pl.BlockSpec(memory_space=pltpu.VMEM)
    dma = pltpu.SemaphoreType.DMA
    flops = 2 * tile_rows * tile_cols * tokens
    og_all, acts_t, kept, new_row, new_col, rs, cs = pl.pallas_call(
        functools.partial(gather_kernel, rows, cols),
        out_shape=(
            jax.ShapeDtypeStruct((n, tokens, width), bf16),
            jax.ShapeDtypeStruct((tile_rows, tokens), bf16),
            jax.ShapeDtypeStruct((n, blocks, KEPT, width), f32),
            jax.ShapeDtypeStruct((1, tile_rows), f32),
            jax.ShapeDtypeStruct((n, 1, width), f32),
            jax.ShapeDtypeStruct((tile_rows, 128), f32),
            jax.ShapeDtypeStruct((n, 1, width), f32),
        ),
        in_specs=[any_space, any_space, any_space, vmem, vmem],
        out_specs=(any_space, any_space, any_space, vmem, vmem, vmem, vmem),
        scratch_shapes=[
            pltpu.VMEM((n, tokens, width), bf16),
            pltpu.VMEM((cols, part, tile_rows), bf16),
            pltpu.VMEM((tile_rows, tokens), bf16),
            pltpu.VMEM((SLOTS, blocks, TALL, width), f32),
            pltpu.VMEM((2, tile_rows // n, tile_cols), bf16),
            pltpu.VMEM((tile_rows, 128), f32),
            pltpu.VMEM((tile_rows, 128), f32),
            pltpu.VMEM((8, 1024), f32),
            pltpu.VMEM((rows, n, 1, width), f32),
            pltpu.VMEM((cols, 1, tile_rows), f32),
            pltpu.VMEM((cols, 2, 128), f32),
            pltpu.VMEM((rows, 3, 128), f32),
            dma((n,)), dma((2, 4, n)), dma((2, cols // 2)), dma((2, cols // 2)), dma((2, rows, n)),
            dma((2, cols)), dma((2, cols)), dma((2, rows)), dma((2,)), dma((n,)), dma((SLOTS,)), dma((2,)),
        ],
        compiler_params=pltpu.CompilerParams(
            collective_id=0, has_side_effects=True, vmem_limit_bytes=62 * 1024 * 1024),
        cost_estimate=pl.CostEstimate(flops=flops, bytes_accessed=2 * weight.size, transcendentals=0),
        name="gather_stats",
    )(activations, output_grads, weight, row_moment.reshape(1, tile_rows), col_moment.reshape(n, 1, width))
    new_weight = pl.pallas_call(
        update_kernel,
        grid=(n, blocks),
        out_shape=jax.ShapeDtypeStruct((tile_rows, tile_cols), bf16),
        in_specs=[
            pl.BlockSpec((tile_rows, tokens), lambda j, i: (0, 0)),
            pl.BlockSpec((1, tokens, width), lambda j, i: (j, 0, 0)),
            pl.BlockSpec((TALL, width), lambda j, i: (i, j)),
            pl.BlockSpec((1, 1, KEPT, width), lambda j, i: (j, i, 0, 0)),
            pl.BlockSpec((TALL, 128), lambda j, i: (i, 0)),
            pl.BlockSpec((1, 1, width), lambda j, i: (j, 0, 0)),
        ],
        out_specs=pl.BlockSpec((TALL, width), lambda j, i: (i, j)),
        compiler_params=pltpu.CompilerParams(
            dimension_semantics=("arbitrary", "arbitrary"), vmem_limit_bytes=48 * 1024 * 1024),
        cost_estimate=pl.CostEstimate(flops=flops, bytes_accessed=4 * weight.size, transcendentals=0),
        name="update_weight",
    )(acts_t, og_all, weight, kept, rs, cs)
    return new_weight, new_row.reshape(tile_rows), new_col.reshape(tile_cols)


def plain(activations, output_grads, weight, row_moment, col_moment):
    tile_rows, tile_cols = weight.shape
    total_rows = tile_rows * lax.axis_size("row")
    total_cols = tile_cols * lax.axis_size("col")
    entries = float(total_rows * total_cols)
    weight_wide = weight.astype(jnp.float32)
    weight_local = jnp.sum(weight_wide * weight_wide)
    weight_total = lax.psum(weight_local, ("row", "col"))
    contract = (((0,), (0,)), ((), ()))
    acts_all = lax.all_gather(activations, "col", axis=0, tiled=True)
    gradient = lax.dot_general(
        acts_all,
        lax.all_gather(output_grads, "row", axis=0, tiled=True),
        contract,
        preferred_element_type=jnp.float32,
    )
    squared = gradient * gradient
    row_part = jnp.sum(squared + ADDED_SQUARE, axis=1)
    col_part = jnp.sum(squared + ADDED_SQUARE, axis=0)
    row_total = lax.psum(row_part, "col")
    col_total = lax.psum(col_part, "row")
    new_row = DECAY_RATE * row_moment + (1.0 - DECAY_RATE) * row_total / total_cols
    new_col = DECAY_RATE * col_moment + (1.0 - DECAY_RATE) * col_total / total_rows
    inverse = lax.rsqrt(new_row[:, None] * new_col[None, :])
    ratio_local = jnp.sum(squared * inverse * inverse)
    leader = (lax.axis_index("col") == 0).astype(jnp.float32)
    row_local = leader * jnp.sum(new_row)
    row_sum, ratio_sum = lax.psum((row_local, ratio_local), ("row", "col"))
    row_mean = row_sum / total_rows
    rms_update = jnp.sqrt(row_mean * ratio_sum / entries)
    clip_factor = jnp.maximum(1.0, rms_update / CLIP_LIMIT)
    step_scale = STEP_SIZE * jnp.sqrt(weight_total / entries + MEAN_OFFSET)
    update = gradient * inverse * jnp.sqrt(row_mean)
    new_weight = (weight_wide - step_scale / clip_factor * update).astype(jnp.bfloat16)
    return (new_weight, new_row, new_col)


def on_device(rows, cols, activations, output_grads, weight, row_moment, col_moment):
    tile_rows, tile_cols = weight.shape
    chunks = tile_cols // WIDTH
    fits = (
        rows == 4 and cols % 2 == 0 and cols > 2
        and tile_rows % TALL == 0 and tile_cols % 1024 == 0
        and chunks > ACTS_READY + SLOTS and tile_rows % (16 * chunks) == 0
        and output_grads.shape[0] % 32 == 0 and activations.shape[0] % 128 == 0
    )
    args = (activations, output_grads, weight, row_moment, col_moment)
    return with_kernels(rows, cols, *args) if fits else plain(*args)


def solution(mesh):
    return jax.shard_map(
        functools.partial(on_device, mesh.shape["row"], mesh.shape["col"]),
        mesh=mesh,
        in_specs=(P("col", "row"), P("row", "col"), P("row", "col"), P("row"), P("col")),
        out_specs=(P("row", "col"), P("row"), P("col")),
        check_vma=False,
    )
```

```python
import functools

import jax
import jax.numpy as jnp
from jax import lax
from jax.experimental import pallas as pl
from jax.experimental.pallas import tpu as pltpu
from jax.sharding import PartitionSpec as P

ADDED_SQUARE = 1e-30
DECAY_RATE = 0.8
CLIP_LIMIT = 1.0
STEP_SIZE = 0.1
MEAN_OFFSET = 1e-06

MESH = pl.DeviceIdType.MESH
WIDTH = 512
BLOCKS = 1
KEEP = 2
DOTS = 1
PIECES = 3
AHEAD = 3
LAG = 2
SLOTS = LAG + 1
ACTS_FORWARD = 4
ACTS_READY = 6


def lane_sum(x):
    out = x[:, :128]
    for k in range(1, x.shape[1] // 128):
        out = out + x[:, k * 128 : (k + 1) * 128]
    return out


def sublane_sum(x):
    return jnp.sum(x.reshape(x.shape[0] // 8, 8, x.shape[1]), axis=0)


def gather_kernel(
    rows, cols,
    acts_ref, og_ref, w_ref, rm_ref, cm_ref,
    og_out, at_out, g_out, nr_out, nc_out, rs_out, cs_out,
    og_all, acts_all, acts_t, grad, wbuf, rowacc, sacc, wacc, colx, rowx, scb, scc,
    load_sem, og_sem, acts_sem, sib_sem, col_sem, row_sem, scb_sem, scc_sem, w_sem, out_sem, g_sem, misc_sem,
):
    n, tokens, width = og_all.shape
    tile_rows = acts_t.shape[0]
    tall = grad.shape[2]
    kept = tall // KEEP
    sub = tile_rows // PIECES
    blocks = tile_rows // tall
    share = tokens // rows
    half = share // 2
    wrows = tile_rows // n
    total_rows = tile_rows * rows
    total_cols = n * width * cols
    entries = float(total_rows * total_cols)
    r, c = lax.axis_index("row"), lax.axis_index("col")
    rx = r + 1 - 2 * lax.rem(r, 2)
    ry = lax.rem(r + 2, 4)
    rd = lax.rem(rx + 2, 4)
    sib = c + 1 - 2 * lax.rem(c, 2)

    def region(owner, start, size):
        return pl.ds(pl.multiple_of(owner * share + start, half), size)

    def load(j):
        return pltpu.make_async_copy(
            og_ref.at[:, pl.ds(pl.multiple_of(j * width, width), width)],
            og_all.at[j, region(r, 0, share), :], load_sem.at[j])

    def og_copy(j, kind, owner, start, size, to):
        ref = og_all.at[j, region(owner, start, size), :]
        return pltpu.make_async_remote_copy(
            src_ref=ref, dst_ref=ref, send_sem=og_sem.at[0, kind, j], recv_sem=og_sem.at[1, kind, j],
            device_id={"row": to}, device_id_type=MESH)

    def own_x(j):
        return og_copy(j, 0, r, 0, share, rx)

    def own_y(j):
        return og_copy(j, 1, r, 0, share, ry)

    def fwd_y(j):
        return og_copy(j, 2, rx, 0, half, ry)

    def fwd_x(j):
        return og_copy(j, 3, ry, half, half, rx)

    def acts_copy(d):
        to = lax.rem(c + 2 * d, cols)
        return pltpu.make_async_remote_copy(
            src_ref=acts_all.at[c], dst_ref=acts_all.at[c], send_sem=acts_sem.at[0, d], recv_sem=acts_sem.at[1, d],
            device_id={"col": to}, device_id_type=MESH)

    def sib_copy(d):
        at = lax.rem(c + cols - 2 * d, cols)
        return pltpu.make_async_remote_copy(
            src_ref=acts_all.at[at], dst_ref=acts_all.at[at], send_sem=sib_sem.at[0, d], recv_sem=sib_sem.at[1, d],
            device_id={"col": sib}, device_id_type=MESH)

    def col_copy(j, d):
        return pltpu.make_async_remote_copy(
            src_ref=colx.at[r, j], dst_ref=colx.at[r, j], send_sem=col_sem.at[0, d, j], recv_sem=col_sem.at[1, d, j],
            device_id={"row": lax.rem(r + d, rows)}, device_id_type=MESH)

    def row_copy(d):
        return pltpu.make_async_remote_copy(
            src_ref=rowx.at[c], dst_ref=rowx.at[c], send_sem=row_sem.at[0, d], recv_sem=row_sem.at[1, d],
            device_id={"col": lax.rem(c + d, cols)}, device_id_type=MESH)

    def scb_copy(d):
        return pltpu.make_async_remote_copy(
            src_ref=scb.at[c], dst_ref=scb.at[c], send_sem=scb_sem.at[0, d], recv_sem=scb_sem.at[1, d],
            device_id={"col": lax.rem(c + d, cols)}, device_id_type=MESH)

    def scc_copy(d):
        return pltpu.make_async_remote_copy(
            src_ref=scc.at[r], dst_ref=scc.at[r], send_sem=scc_sem.at[0, d], recv_sem=scc_sem.at[1, d],
            device_id={"row": lax.rem(r + d, rows)}, device_id_type=MESH)

    def w_copy(j):
        return pltpu.make_async_copy(
            w_ref.at[pl.ds(pl.multiple_of(j * wrows, wrows), wrows), :], wbuf.at[lax.rem(j, 2)], w_sem.at[lax.rem(j, 2)])

    def og_store(j):
        return pltpu.make_async_copy(og_all.at[j], og_out.at[j], out_sem.at[j])

    def g_store(j):
        s = lax.rem(j, SLOTS)
        return pltpu.make_async_copy(grad.at[s, :, pl.ds(tall - kept, kept), :], g_out.at[j], g_sem.at[s])

    acts_load = pltpu.make_async_copy(acts_ref, acts_all.at[c], misc_sem.at[0])
    acts_store = pltpu.make_async_copy(acts_t, at_out, misc_sem.at[1])

    acts_load.start()

    @pl.loop(0, n)
    def _(j):
        load(j).start()

    w_copy(0).start()
    w_copy(1).start()

    barrier = pltpu.get_barrier_semaphore()
    for d in range(1, rows):
        pl.semaphore_signal(barrier, inc=1, device_id={"row": lax.rem(r + d, rows)}, device_id_type=MESH)
    for d in range(1, cols):
        pl.semaphore_signal(barrier, inc=1, device_id={"col": lax.rem(c + d, cols)}, device_id_type=MESH)
    rowacc[...] = jnp.zeros_like(rowacc)
    sacc[...] = jnp.zeros_like(sacc)
    wacc[...] = jnp.zeros_like(wacc)
    pl.semaphore_wait(barrier, rows + cols - 2)

    def send_own(j):
        load(j).wait()
        own_x(j).start()
        own_y(j).start()

    for j in range(AHEAD):
        send_own(j)
    acts_load.wait()
    for d in range(1, cols // 2):
        acts_copy(d).start()
    sib_copy(0).start()

    def exchange(j):
        own_x(j).wait_recv()
        fwd_y(j).start()
        own_y(j).wait_recv()
        fwd_x(j).start()

        @pl.when(j + AHEAD < n)
        def _():
            send_own(j + AHEAD)

    def weigh(j):
        w_copy(j).wait()
        s = lax.rem(j, 2)
        wide = 1024

        @pl.loop(0, wbuf.shape[2] // wide)
        def _(k):
            x = wbuf[s, :, pl.ds(pl.multiple_of(k * wide, wide), wide)].astype(jnp.float32)
            wacc[...] += sublane_sum(x * x)

        @pl.when(j + 2 < n)
        def _():
            w_copy(j + 2).start()

    def stats(k):
        for d in range(1, rows):
            col_copy(k, d).wait_recv()
        total = colx[0, k]
        for q in range(1, rows):
            total = total + colx[q, k]
        factor = DECAY_RATE * cm_ref[k] + (1.0 - DECAY_RATE) * total / total_rows
        nc_out[k] = factor
        cs_out[k] = lax.rsqrt(factor)
        weight = 1.0 / factor
        s = lax.rem(k, SLOTS)
        for b in range(blocks):
            @pl.loop(0, tall // sub)
            def _(i):
                at = pl.ds(pl.multiple_of(i * sub, sub), sub)
                g = grad[s, b, at, :]
                to = pl.ds(pl.multiple_of(b * tall + i * sub, sub), sub)
                sacc[to, :] += lane_sum(g * g * weight)

    def compute(k):
        fwd_y(k).wait_recv()
        fwd_x(k).wait_recv()
        og_store(k).start()
        s = lax.rem(k, SLOTS)

        @pl.when(k >= SLOTS)
        def _():
            g_store(k - SLOTS).wait()

        right = og_all.at[k]
        column = jnp.zeros((8, width), jnp.float32)
        for b in range(blocks):
            def step(i, column):
                to = pl.ds(pl.multiple_of(b * tall + i * sub, sub), sub)
                g = jnp.dot(acts_t[to, :], right[...], preferred_element_type=jnp.float32)
                grad[s, b, pl.ds(pl.multiple_of(i * sub, sub), sub), :] = g
                squared = g * g + ADDED_SQUARE
                rowacc[to, :] += lane_sum(squared)
                return column + sublane_sum(squared)
            column = lax.fori_loop(0, tall // sub, step, column)
        colx[r, k] = jnp.sum(column, axis=0, keepdims=True)
        for d in range(1, rows):
            col_copy(k, d).start()
        g_store(k).start()

        @pl.when(k >= LAG)
        def _():
            stats(k - LAG)

    def reach(j):
        return jnp.minimum(j, 2 * (j - ACTS_READY + 1))

    @pl.loop(0, ACTS_FORWARD)
    def _(j):
        exchange(j)
        weigh(j)

    for d in range(1, cols // 2):
        acts_copy(d).wait_recv()
        sib_copy(d).start()

    @pl.loop(ACTS_FORWARD, ACTS_READY)
    def _(j):
        exchange(j)
        weigh(j)

    for d in range(cols // 2):
        sib_copy(d).wait_recv()
    part = acts_all.shape[1]
    for q in range(cols):
        acts_t[:, q * part : (q + 1) * part] = acts_all[q].T
    acts_store.start()

    @pl.loop(ACTS_READY, n)
    def _(j):
        exchange(j)
        weigh(j)

        @pl.loop(reach(j - 1), reach(j))
        def _(k):
            compute(k)

    @pl.loop(n - 1, n)
    def _(k):
        compute(k)

    rowx[c] = jnp.sum(rowacc[...].T, axis=0, keepdims=True)
    for d in range(1, cols):
        row_copy(d).start()

    @pl.loop(n - LAG, n)
    def _(k):
        stats(k)

    ratio_rows = jnp.sum(sacc[...].T, axis=0, keepdims=True)
    for d in range(1, cols):
        row_copy(d).wait_recv()
    row_total = rowx[0]
    for q in range(1, cols):
        row_total = row_total + rowx[q]
    new_row = DECAY_RATE * rm_ref[...] + (1.0 - DECAY_RATE) * row_total / total_cols
    nr_out[...] = new_row

    def spread(x):
        return jnp.broadcast_to(jnp.sum(x, axis=1, keepdims=True), (1, 128))

    scb[c, 0:1, :] = spread(ratio_rows / new_row)
    scb[c, 1:2, :] = spread(jnp.sum(wacc[...], axis=0, keepdims=True))
    for d in range(1, cols):
        scb_copy(d).start()
    row_sum = spread(new_row)
    for d in range(1, cols):
        scb_copy(d).wait_recv()
    both = scb[0]
    for q in range(1, cols):
        both = both + scb[q]
    scc[r, 0:2, :] = both[0:2, :]
    scc[r, 2:3, :] = row_sum
    for d in range(1, rows):
        scc_copy(d).start()
    root = lax.rsqrt(new_row)
    for d in range(1, rows):
        scc_copy(d).wait_recv()
    every = scc[0]
    for q in range(1, rows):
        every = every + scc[q]
    row_mean = every[2:3, :] / total_rows
    rms_update = jnp.sqrt(row_mean * (every[0:1, :] / entries))
    clip_factor = jnp.maximum(1.0, rms_update / CLIP_LIMIT)
    step_scale = STEP_SIZE * jnp.sqrt(every[1:2, :] / entries + MEAN_OFFSET)
    scale = step_scale / clip_factor * jnp.sqrt(row_mean)
    rs_out[...] = jnp.broadcast_to(root, (128, tile_rows)).T * scale

    @pl.loop(0, n)
    def _(j):
        own_x(j).wait_send()
        own_y(j).wait_send()
        fwd_y(j).wait_send()
        fwd_x(j).wait_send()
        og_store(j).wait()
        for d in range(1, rows):
            col_copy(j, d).wait_send()

    @pl.loop(n - SLOTS, n)
    def _(j):
        g_store(j).wait()

    acts_store.wait()
    for d in range(1, cols // 2):
        acts_copy(d).wait_send()
    for d in range(cols // 2):
        sib_copy(d).wait_send()
    for d in range(1, cols):
        row_copy(d).wait_send()
        scb_copy(d).wait_send()
    for d in range(1, rows):
        scc_copy(d).wait_send()


def update_kernel(at_ref, og_ref, w_ref, g_ref, rs_ref, cs_ref, out_ref):
    i = pl.program_id(1)
    tall, width = w_ref.shape
    j = pl.program_id(0)
    cs = cs_ref[j]
    kept = tall // KEEP
    sub = (tall - kept) // DOTS

    def finish(g, at):
        rs = rs_ref[pl.ds(pl.multiple_of(i * tall + at.start, 16), at.size), :]
        wide = jnp.concatenate([rs] * (width // 128), axis=1)
        out_ref[at, :] = (w_ref[at, :].astype(jnp.float32) - g * wide * cs).astype(out_ref.dtype)

    finish(g_ref[0, 0], pl.ds(tall - kept, kept))
    for k in range(DOTS):
        left = at_ref[pl.ds(pl.multiple_of(i * tall + k * sub, 16), sub), :]
        g = jnp.dot(left, og_ref[0], preferred_element_type=jnp.float32)
        finish(g, pl.ds(k * sub, sub))


def with_kernels(rows, cols, activations, output_grads, weight, row_moment, col_moment):
    tile_rows, tile_cols = weight.shape
    part = activations.shape[0]
    tokens = part * cols
    n, width = tile_cols // WIDTH, WIDTH
    blocks = BLOCKS
    tall = tile_rows // blocks
    kept = tall // KEEP
    f32, bf16 = jnp.float32, jnp.bfloat16
    any_space = pl.BlockSpec(memory_space=pl.ANY)
    vmem = pl.BlockSpec(memory_space=pltpu.VMEM)
    dma = pltpu.SemaphoreType.DMA
    flops = 2 * tile_rows * tile_cols * tokens
    og_all, acts_t, grads, new_row, new_col, rs, cs = pl.pallas_call(
        functools.partial(gather_kernel, rows, cols),
        out_shape=(
            jax.ShapeDtypeStruct((n, tokens, width), bf16),
            jax.ShapeDtypeStruct((tile_rows, tokens), bf16),
            jax.ShapeDtypeStruct((n, blocks, kept, width), f32),
            jax.ShapeDtypeStruct((1, tile_rows), f32),
            jax.ShapeDtypeStruct((n, 1, width), f32),
            jax.ShapeDtypeStruct((tile_rows, 128), f32),
            jax.ShapeDtypeStruct((n, 1, width), f32),
        ),
        in_specs=[any_space, any_space, any_space, vmem, vmem],
        out_specs=(any_space, any_space, any_space, vmem, vmem, vmem, vmem),
        scratch_shapes=[
            pltpu.VMEM((n, tokens, width), bf16),
            pltpu.VMEM((cols, part, tile_rows), bf16),
            pltpu.VMEM((tile_rows, tokens), bf16),
            pltpu.VMEM((SLOTS, blocks, tall, width), f32),
            pltpu.VMEM((2, tile_rows // n, tile_cols), bf16),
            pltpu.VMEM((tile_rows, 128), f32),
            pltpu.VMEM((tile_rows, 128), f32),
            pltpu.VMEM((8, 1024), f32),
            pltpu.VMEM((rows, n, 1, width), f32),
            pltpu.VMEM((cols, 1, tile_rows), f32),
            pltpu.VMEM((cols, 2, 128), f32),
            pltpu.VMEM((rows, 3, 128), f32),
            dma((n,)), dma((2, 4, n)), dma((2, cols // 2)), dma((2, cols // 2)), dma((2, rows, n)),
            dma((2, cols)), dma((2, cols)), dma((2, rows)), dma((2,)), dma((n,)), dma((SLOTS,)), dma((2,)),
        ],
        compiler_params=pltpu.CompilerParams(
            collective_id=0, has_side_effects=True, vmem_limit_bytes=62 * 1024 * 1024),
        cost_estimate=pl.CostEstimate(flops=flops, bytes_accessed=2 * weight.size, transcendentals=0),
        name="gather_stats",
    )(activations, output_grads, weight, row_moment.reshape(1, tile_rows), col_moment.reshape(n, 1, width))
    new_weight = pl.pallas_call(
        update_kernel,
        grid=(n, blocks),
        out_shape=jax.ShapeDtypeStruct((tile_rows, tile_cols), bf16),
        in_specs=[
            pl.BlockSpec((tile_rows, tokens), lambda j, i: (0, 0)),
            pl.BlockSpec((1, tokens, width), lambda j, i: (j, 0, 0)),
            pl.BlockSpec((tall, width), lambda j, i: (i, j)),
            pl.BlockSpec((1, 1, kept, width), lambda j, i: (j, i, 0, 0)),
            vmem,
            vmem,
        ],
        out_specs=pl.BlockSpec((tall, width), lambda j, i: (i, j)),
        compiler_params=pltpu.CompilerParams(
            dimension_semantics=("arbitrary", "arbitrary"), vmem_limit_bytes=48 * 1024 * 1024),
        cost_estimate=pl.CostEstimate(flops=flops, bytes_accessed=4 * weight.size, transcendentals=0),
        name="update_weight",
    )(acts_t, og_all, weight, grads, rs, cs)
    return new_weight, new_row.reshape(tile_rows), new_col.reshape(tile_cols)


def plain(activations, output_grads, weight, row_moment, col_moment):
    tile_rows, tile_cols = weight.shape
    total_rows = tile_rows * lax.axis_size("row")
    total_cols = tile_cols * lax.axis_size("col")
    entries = float(total_rows * total_cols)
    weight_wide = weight.astype(jnp.float32)
    weight_local = jnp.sum(weight_wide * weight_wide)
    weight_total = lax.psum(weight_local, ("row", "col"))
    contract = (((0,), (0,)), ((), ()))
    acts_all = lax.all_gather(activations, "col", axis=0, tiled=True)
    gradient = lax.dot_general(
        acts_all,
        lax.all_gather(output_grads, "row", axis=0, tiled=True),
        contract,
        preferred_element_type=jnp.float32,
    )
    squared = gradient * gradient
    row_part = jnp.sum(squared + ADDED_SQUARE, axis=1)
    col_part = jnp.sum(squared + ADDED_SQUARE, axis=0)
    row_total = lax.psum(row_part, "col")
    col_total = lax.psum(col_part, "row")
    new_row = DECAY_RATE * row_moment + (1.0 - DECAY_RATE) * row_total / total_cols
    new_col = DECAY_RATE * col_moment + (1.0 - DECAY_RATE) * col_total / total_rows
    inverse = lax.rsqrt(new_row[:, None] * new_col[None, :])
    ratio_local = jnp.sum(squared * inverse * inverse)
    leader = (lax.axis_index("col") == 0).astype(jnp.float32)
    row_local = leader * jnp.sum(new_row)
    row_sum, ratio_sum = lax.psum((row_local, ratio_local), ("row", "col"))
    row_mean = row_sum / total_rows
    rms_update = jnp.sqrt(row_mean * ratio_sum / entries)
    clip_factor = jnp.maximum(1.0, rms_update / CLIP_LIMIT)
    step_scale = STEP_SIZE * jnp.sqrt(weight_total / entries + MEAN_OFFSET)
    update = gradient * inverse * jnp.sqrt(row_mean)
    new_weight = (weight_wide - step_scale / clip_factor * update).astype(jnp.bfloat16)
    return (new_weight, new_row, new_col)


def on_device(rows, cols, activations, output_grads, weight, row_moment, col_moment):
    tile_rows, tile_cols = weight.shape
    chunks = tile_cols // WIDTH
    fits = (
        rows == 4 and cols % 2 == 0 and cols > 2
        and tile_rows % (64 * BLOCKS * KEEP * DOTS) == 0 and tile_rows % (16 * BLOCKS * PIECES) == 0 and tile_cols % 1024 == 0
        and chunks > ACTS_READY + SLOTS and tile_rows % (16 * chunks) == 0
        and output_grads.shape[0] % 32 == 0 and activations.shape[0] % 128 == 0
    )
    args = (activations, output_grads, weight, row_moment, col_moment)
    return with_kernels(rows, cols, *args) if fits else plain(*args)


def solution(mesh):
    return jax.shard_map(
        functools.partial(on_device, mesh.shape["row"], mesh.shape["col"]),
        mesh=mesh,
        in_specs=(P("col", "row"), P("row", "col"), P("row", "col"), P("row"), P("col")),
        out_specs=(P("row", "col"), P("row"), P("col")),
        check_vma=False,
    )
```
